32 devices in a mesh: section: 4 (over z), dp: 8 (over y, x, core).
Axes of the slice: x: 2, y: 2, z: 4, core: 2. Of those that a mesh axis runs over, the one named last changes fastest.
Arguments:
- stream: float32 [2, 64, 16, 16, 128], P(None, 'dp'), may hold values from -6 to 6
- cotangent: float32 [2, 64, 16, 16, 128], P(None, 'dp'), may hold values from -6 to 6
- weights: bfloat16 [4, 2304, 128], P('section'), may hold values from -0.09375 to 0.09375
- master: float32 [4, 2304, 128], P('section', 'dp'), may hold values from -0.09375 to 0.09375
- momentum: float32 [4, 2304, 128], P('section', 'dp'), may hold values from -6 to 6
Outputs:
- new_master: float32 [4, 2304, 128], P('section', 'dp')
- new_momentum: float32 [4, 2304, 128], P('section', 'dp')
- new_weights: bfloat16 [4, 2304, 128], P('section')
The draws below stay inside these ranges and needn't reach their ends.
All inputs are finite; a program needn't handle non-finite values.
Results may differ from the reference program's by a relative error of at most 0.014.
Values may be sent and summed in bfloat16 or wider, within the bound.
A program may use at most 64 MiB of HBM per device.

```python
import jax
import jax.numpy as jnp
from jax import lax

C = 128
SIDE = 16
LAYERS = 1
SECTIONS = 4
IMAGES = 64
ROWS = 2304
N_SECTION = 4


def block_levels(own_key, shape, cuts, least, largest):
    loudness, own = 1.0, jax.random.fold_in(own_key, 6)
    for dim, parts in cuts:
        heights = jnp.exp(jax.random.uniform(jax.random.fold_in(own, dim), (parts,), jnp.float32, least / len(cuts), largest / len(cuts)))
        loudness = loudness * jnp.repeat(heights, shape[dim] // parts).reshape([-1 if axis == dim else 1 for axis in range(len(shape))])
    return loudness


def scatter_about(key, extent, scale, most, split=(), held_as=jnp.bfloat16):
    level = block_levels(key, extent, split, -0.22, 0.18) if split else 1.0
    entries = jax.random.normal(key, extent, jnp.float32) * scale * level
    return jnp.minimum(jnp.maximum(entries, -most), most).astype(held_as)


def setup_inputs(seed: int = 0) -> dict:
    seeds = jax.random.split(jax.random.key(seed), 6)
    stream = scatter_about(seeds[0], (2, IMAGES, SIDE, SIDE, C), 1.0, 6.0, ((1, 8),), jnp.float32)
    cotangent = scatter_about(seeds[1], (2, IMAGES, SIDE, SIDE, C), 1.0, 6.0, ((1, 8),), jnp.float32)
    weights = scatter_about(seeds[2], (SECTIONS, ROWS, C), (36 * C) ** -0.5, 0.09375, ((0, 4),))
    master = scatter_about(seeds[3], (SECTIONS, ROWS, C), (36 * C) ** -0.5, 0.09375, ((0, 4), (1, 8)), jnp.float32)
    momentum = scatter_about(seeds[4], (SECTIONS, ROWS, C), 1.0, 6.0, ((0, 4), (1, 8)), jnp.float32)
    return dict(stream=stream, cotangent=cotangent, weights=weights, master=master, momentum=momentum)


step_size = 0.1
inertia = 0.9

def product(left_op, right_op, dims):
    return lax.dot_general(left_op.astype(jnp.float32), right_op.astype(jnp.float32), (dims, ((), ())), precision=lax.Precision.HIGHEST, preferred_element_type=jnp.float32)

def columns(field):
    height = field.shape[1]
    breadth = field.shape[2]
    padded = jnp.pad(jax.nn.silu(field).astype(jnp.bfloat16), ((0, 0), (1, 1), (1, 1), (0, 0)))
    shifted = [padded[:, row_tap:row_tap + height, col_tap:col_tap + breadth, :] for row_tap in range(3) for col_tap in range(3)]
    return jnp.concatenate(shifted, axis=3).reshape(-1, 9 * field.shape[3])

def convolve(patches, weight, template):
    return product(patches, weight, ((1,), (0,))).reshape(template.shape)

def spread(rounded, weight, template):
    height, breadth, channels = (template.shape[1], template.shape[2], template.shape[3])
    spread_cols = product(rounded, weight, ((1,), (1,))).reshape(template.shape[0], height, breadth, 9 * channels)
    padded = jnp.pad(spread_cols, ((0, 0), (1, 1), (1, 1), (0, 0)))
    summed = jnp.zeros(template.shape, jnp.float32)
    for row_tap in range(3):
        for col_tap in range(3):
            tap_index = 3 * row_tap + col_tap
            summed = summed + padded[:, 2 - row_tap:2 - row_tap + height, 2 - col_tap:2 - col_tap + breadth, tap_index * channels:(tap_index + 1) * channels]
    return summed

def weight_grad(patches, rounded):
    return product(patches, rounded, ((0,), (0,)))

def silu_slope(field):
    logistic = jax.nn.sigmoid(field)
    return logistic * (1.0 + field * (1.0 - logistic))

def coupling_forward(first, second, weight_f, weight_g):
    patch_f = columns(second)
    out_first = first + convolve(patch_f, weight_f, second)
    patch_g = columns(out_first)
    out_second = second + convolve(patch_g, weight_g, out_first)
    return (out_first, out_second)

def coupling_backward(out_first, out_second, grad_first, grad_second, weight_f, weight_g):
    channels = out_first.shape[3]
    patch_g = columns(out_first)
    second = out_second - convolve(patch_g, weight_g, out_first)
    patch_f = columns(second)
    first = out_first - convolve(patch_f, weight_f, second)
    round_second = grad_second.astype(jnp.bfloat16).reshape(-1, channels)
    wgrad_g = weight_grad(patch_g, round_second)
    grad_first = grad_first + spread(round_second, weight_g, out_first) * silu_slope(out_first)
    round_first = grad_first.astype(jnp.bfloat16).reshape(-1, channels)
    wgrad_f = weight_grad(patch_f, round_first)
    grad_second = grad_second + spread(round_first, weight_f, second) * silu_slope(second)
    return (first, second, grad_first, grad_second, wgrad_f, wgrad_g)

def reference(stream, cotangent, weights, master, momentum):
    blocks = weights.reshape(N_SECTION, LAYERS, 2, 9 * C, C)
    first, second = (stream[0], stream[1])
    for section_idx in range(N_SECTION):
        for coupling in range(LAYERS):
            first, second = coupling_forward(first, second, blocks[section_idx, coupling, 0], blocks[section_idx, coupling, 1])
    grad_first, grad_second = (cotangent[0], cotangent[1])
    section_grads = []
    for section_idx in reversed(range(N_SECTION)):
        pieces = []
        for coupling in reversed(range(LAYERS)):
            first, second, grad_first, grad_second, wgrad_f, wgrad_g = coupling_backward(first, second, grad_first, grad_second, blocks[section_idx, coupling, 0], blocks[section_idx, coupling, 1])
            pieces.append(jnp.stack([wgrad_f, wgrad_g]))
        pieces = pieces[::-1]
        section_grads.append(jnp.stack(pieces).reshape(LAYERS * 18 * C, C))
    section_grads = section_grads[::-1]
    gradient = jnp.stack(section_grads) / IMAGES
    new_momentum = inertia * momentum + gradient
    new_master = master - step_size * new_momentum
    return (new_master, new_momentum, new_master.astype(jnp.bfloat16))
```

```python
import functools

import jax
import jax.numpy as jnp
from jax import lax
from jax.experimental import pallas as pl
from jax.experimental.pallas import tpu as pltpu
from jax.sharding import PartitionSpec as P

MESH = pl.DeviceIdType.MESH
step_size = 0.1
inertia = 0.9


def kernel(
    S, D, images,
    stream, cotangent, weights, master, momentum,
    new_master, new_momentum, new_weights,
    wbuf, xs, ds, pads, kept, slopes, g32, gsend, recv1, zsend, recv2, gown, wsend,
    in_sem, own_sem, wsend_sem, wrecv_sem, fsend_sem, frecv_sem,
    gsend_sem, grecv_sem, zsend_sem, zrecv_sem, osend_sem, orecv_sem,
):
    s = lax.axis_index("section")
    d = lax.axis_index("dp")
    half = lax.rem(d, 2)
    partner = d + 1 - 2 * half
    share, H, W, C = xs.shape[1:]
    M = share * H * W
    rows = master.shape[0]

    def weight_copy(sec_from, to):
        return pltpu.make_async_remote_copy(
            src_ref=weights.at[half], dst_ref=wbuf.at[sec_from, half],
            send_sem=wsend_sem.at[to], recv_sem=wrecv_sem.at[sec_from],
            device_id=(to, d), device_id_type=MESH)

    def forward_copy(sec, which):
        return pltpu.make_async_remote_copy(
            src_ref=wbuf.at[sec, which], dst_ref=wbuf.at[sec, which],
            send_sem=fsend_sem.at[sec], recv_sem=frecv_sem.at[sec],
            device_id=(s, partner), device_id_type=MESH)

    for i in range(1, S):
        weight_copy(s, lax.rem(s + i, S)).start()
    load_own = pltpu.make_async_copy(weights, wbuf.at[s], own_sem)
    load_own.start()
    mine = pl.ds(s * share, share)
    loads = [
        pltpu.make_async_copy(stream.at[0, mine], xs.at[0], in_sem.at[0]),
        pltpu.make_async_copy(stream.at[1, mine], xs.at[1], in_sem.at[1]),
        pltpu.make_async_copy(cotangent.at[0, mine], ds.at[0], in_sem.at[2]),
        pltpu.make_async_copy(cotangent.at[1, mine], ds.at[1], in_sem.at[3]),
    ]
    for load in loads:
        load.start()

    zero_row = jnp.zeros((share, 1, W, 3 * C), jnp.bfloat16)
    for k in range(2):
        pads[k, :, 0:1] = zero_row
        pads[k, :, H + 1 : H + 2] = zero_row

    col = lax.rem(lax.broadcasted_iota(jnp.int32, (M, C), 0), W)

    def shifted(k, flat, order):
        before = jnp.where(col == 0, 0.0, pltpu.roll(flat, 1, 0))
        after = jnp.where(col == W - 1, 0.0, pltpu.roll(flat, M - 1, 0))
        for b, piece in enumerate((before, flat, after) if order else (after, flat, before)):
            pads[k, :, 1 : H + 1, :, b * C : (b + 1) * C] = piece.astype(jnp.bfloat16).reshape(
                share, H, W, C)

    def activate(value, sec, which):
        logistic = 1.0 / (1.0 + jnp.exp(-value))
        act = value * logistic
        slopes[sec, which] = logistic * (1.0 + value * (1.0 - logistic))
        kept[sec, which] = act.astype(jnp.bfloat16)
        shifted(0, act, True)

    def conv(sec, which):
        total = jnp.zeros((M, C), jnp.float32)
        for a in range(3):
            total += jnp.dot(
                pads[0, :, a : a + H].reshape(M, 3 * C),
                wbuf[sec, which, a * 3 * C : (a + 1) * 3 * C],
                preferred_element_type=jnp.float32)
        return total

    def pass_on(sec):
        @pl.when(sec != s)
        def _():
            weight_copy(sec, s).wait_recv()
            forward_copy(sec, half).start()

    def take(sec):
        @pl.when(sec != s)
        def _():
            forward_copy(sec, 1 - half).wait_recv()

    load_own.wait()
    for load in loads:
        load.wait()
    pass_on(0)

    def forward_one(sec, carry):
        first = xs[0].reshape(M, C)
        second = xs[1].reshape(M, C)
        activate(second, sec, 0)
        take(sec)
        first = first + conv(sec, 0)
        activate(first, sec, 1)
        xs[0] = first.reshape(share, H, W, C)

        @pl.when(sec + 1 < S)
        def _():
            pass_on(sec + 1)

        xs[1] = (second + conv(sec, 1)).reshape(share, H, W, C)
        return carry

    lax.fori_loop(0, S, forward_one, 0)

    def grad_copy(sec, src, to):
        return pltpu.make_async_remote_copy(
            src_ref=gsend.at[sec, to], dst_ref=recv1.at[sec, src],
            send_sem=gsend_sem.at[sec, to], recv_sem=grecv_sem.at[sec, src],
            device_id=(s, to), device_id_type=MESH)

    def sum_copy(sec, src):
        return pltpu.make_async_remote_copy(
            src_ref=zsend.at[sec], dst_ref=recv2.at[src],
            send_sem=zsend_sem.at[sec], recv_sem=zrecv_sem.at[src],
            device_id=(sec, d), device_id_type=MESH)

    def grads(sec, which):
        rounded = ds[1 if which else 0].reshape(M, C)
        shifted(1, rounded, False)
        act = kept[sec, which]
        for a in range(3):
            block = lax.dot_general(
                act, pads[1, :, 2 - a : 2 - a + H].reshape(M, 3 * C),
                (((0,), (0,)), ((), ())), preferred_element_type=jnp.float32)
            for b in range(3):
                g32[(3 * a + b) * C : (3 * a + b + 1) * C] = block[:, b * C : (b + 1) * C]
        per = D // 2

        def send(i, carry):
            at = lax.rem(i + d, per)
            to = which * per + at
            gsend[sec, to] = g32[pl.ds(pl.multiple_of(at * rows, 8), rows)].astype(jnp.bfloat16)

            @pl.when(to != d)
            def _():
                grad_copy(sec, d, to).start()
            return carry

        lax.fori_loop(0, per, send, 0)
        total = jnp.zeros((M, C), jnp.float32)
        for a in range(3):
            for b in range(3):
                tap = 3 * a + b
                total += lax.dot_general(
                    pads[1, :, 2 - a : 2 - a + H, :, b * C : (b + 1) * C].reshape(M, C),
                    wbuf[sec, which, tap * C : (tap + 1) * C],
                    (((1,), (1,)), ((), ())), preferred_element_type=jnp.float32)
        into = 0 if which else 1
        ds[into] = ds[into] + (total * slopes[sec, which]).reshape(share, H, W, C)

    def finish(sec):
        def add(i, total):
            src = lax.rem(d + i, D)
            grad_copy(sec, src, d).wait_recv()
            return total + recv1[sec, src].astype(jnp.float32)

        total = lax.fori_loop(1, D, add, gsend[sec, d].astype(jnp.float32))

        @pl.when(sec == s)
        def _():
            gown[...] = total

        @pl.when(sec != s)
        def _():
            zsend[sec] = total.astype(jnp.bfloat16)
            sum_copy(sec, s).start()

    def backward_one(turn, carry):
        sec = S - 1 - turn
        grads(sec, 1)

        @pl.when(turn > 0)
        def _():
            finish(sec + 1)

        grads(sec, 0)
        return carry

    lax.fori_loop(0, S, backward_one, 0)
    finish(0)

    def gather_sums(i, total):
        src = lax.rem(s + i, S)
        sum_copy(s, src).wait_recv()
        return total + recv2[src].astype(jnp.float32)

    summed = lax.fori_loop(1, S, gather_sums, gown[...])
    moved = inertia * momentum[...] + summed / images
    new_momentum[...] = moved
    fresh = master[...] - step_size * moved
    new_master[...] = fresh
    wsend[...] = fresh.astype(jnp.bfloat16)

    def out_copy(src, to):
        return pltpu.make_async_remote_copy(
            src_ref=wsend, dst_ref=new_weights.at[src],
            send_sem=osend_sem.at[to], recv_sem=orecv_sem.at[src],
            device_id=(s, to), device_id_type=MESH)

    @pl.loop(1, D)
    def _(i):
        out_copy(d, lax.rem(d + i, D)).start()

    keep_own = pltpu.make_async_copy(wsend, new_weights.at[d], own_sem)
    keep_own.start()

    @pl.loop(1, S)
    def _(i):
        other = lax.rem(s + i, S)
        weight_copy(s, other).wait_send()
        forward_copy(other, half).wait_send()
        sum_copy(other, s).wait_send()

    @pl.loop(0, S)
    def _(sec):
        @pl.loop(1, D)
        def _(i):
            grad_copy(sec, d, lax.rem(d + i, D)).wait_send()

    keep_own.wait()

    @pl.loop(1, D)
    def _(i):
        other = lax.rem(d + i, D)
        out_copy(d, other).wait_send()
        out_copy(other, d).wait_recv()


def on_device(S, D, stream, cotangent, weights, master, momentum):
    _, per_dp, H, W, C = stream.shape
    share = per_dp // S
    M = share * H * W
    R = weights.shape[1]
    rows = master.shape[1]
    bf, f32 = jnp.bfloat16, jnp.float32
    vmem = pl.BlockSpec(memory_space=pltpu.VMEM)
    hbm = pl.BlockSpec(memory_space=pl.ANY)
    dma = pltpu.SemaphoreType.DMA
    new_master, new_momentum, new_weights = pl.pallas_call(
        functools.partial(kernel, S, D, per_dp * D),
        out_shape=(
            jax.ShapeDtypeStruct((rows, C), f32),
            jax.ShapeDtypeStruct((rows, C), f32),
            jax.ShapeDtypeStruct((D, rows, C), bf),
        ),
        in_specs=[hbm, hbm, hbm, vmem, vmem],
        out_specs=(vmem, vmem, hbm),
        scratch_shapes=[
            pltpu.VMEM((S, 2, R // 2, C), bf),
            pltpu.VMEM((2, share, H, W, C), f32),
            pltpu.VMEM((2, share, H, W, C), f32),
            pltpu.VMEM((2, share, H + 2, W, 3 * C), bf),
            pltpu.VMEM((S, 2, M, C), bf),
            pltpu.VMEM((S, 2, M, C), f32),
            pltpu.VMEM((R // 2, C), f32),
            pltpu.VMEM((S, D, rows, C), bf),
            pltpu.VMEM((S, D, rows, C), bf),
            pltpu.VMEM((S, rows, C), bf),
            pltpu.VMEM((S, rows, C), bf),
            pltpu.VMEM((rows, C), f32),
            pltpu.VMEM((rows, C), bf),
            dma((4,)), dma, dma((S,)), dma((S,)), dma((S,)), dma((S,)),
            dma((S, D)), dma((S, D)), dma((S,)), dma((S,)), dma((D,)), dma((D,)),
        ],
        compiler_params=pltpu.CompilerParams(
            has_side_effects=True, vmem_limit_bytes=48 * 1024 * 1024),
    )(stream, cotangent, weights.reshape(2, R // 2, C), master[0], momentum[0])
    return (new_master[None], new_momentum[None], new_weights.reshape(1, R, C))


def solution(mesh):
    placed = (
        P(None, "dp", None, None, None),
        P(None, "dp", None, None, None),
        P("section", None, None),
        P("section", "dp", None),
        P("section", "dp", None),
    )
    return jax.shard_map(
        functools.partial(on_device, mesh.shape["section"], mesh.shape["dp"]),
        mesh=mesh,
        in_specs=placed,
        out_specs=(P("section", "dp", None), P("section", "dp", None), P("section", None, None)),
        check_vma=False,
    )
```

```python
import functools
import math

import jax
import jax.numpy as jnp
from jax import lax
from jax.experimental import pallas as pl
from jax.experimental.pallas import tpu as pltpu
from jax.sharding import PartitionSpec as P

MESH = pl.DeviceIdType.MESH
step_size = 0.1
inertia = 0.9


def kernel(
    S, D, images,
    stream, cotangent, weights, master, momentum,
    new_master, new_momentum, new_weights,
    wbuf, xs, ds, pads, kept, slopes, g32, gsend, pairs, recv1, zsend, recv2, gown, spread_out,
    in_sem, own_sem, w1send, w1recv, w2send, w2recv, w3send, w3recv,
    psend, precv, gsend_sem, grecv_sem, zsend_sem, zrecv_sem,
    osend_sem, orecv_sem, fsend_sem, frecv_sem,
):
    s = lax.axis_index("section")
    d = lax.axis_index("dp")
    core = lax.rem(d, 2)
    partner = d + 1 - 2 * core
    chips = D // 2
    share, H, W, C = xs.shape[1:]
    M = share * H * W
    rows = master.shape[0]
    R = rows * D
    NC = math.gcd(R // 16, D)
    part = R // NC

    def chunk(i):
        return pl.ds(pl.multiple_of(i * part, 16), part)

    def other_chip(i):
        return lax.rem(d + 2 * i, D)

    def section_copy(src, to):
        return pltpu.make_async_remote_copy(
            src_ref=weights.at[chunk(d)], dst_ref=wbuf.at[src, chunk(d)],
            send_sem=w1send.at[to], recv_sem=w1recv.at[src],
            device_id=(to, d), device_id_type=MESH)

    def layer_copy(sec, src, to):
        return pltpu.make_async_remote_copy(
            src_ref=wbuf.at[sec, chunk(src)], dst_ref=wbuf.at[sec, chunk(src)],
            send_sem=w2send.at[sec, to], recv_sem=w2recv.at[sec, src],
            device_id=(s, to), device_id_type=MESH)

    def core_copy(sec, src):
        return pltpu.make_async_remote_copy(
            src_ref=wbuf.at[sec, chunk(src)], dst_ref=wbuf.at[sec, chunk(src)],
            send_sem=w3send.at[sec, src], recv_sem=w3recv.at[sec, src],
            device_id=(s, partner), device_id_type=MESH)

    @pl.when(d < NC)
    def _():
        for i in range(1, S):
            section_copy(s, lax.rem(s + i, S)).start()

    load_own = pltpu.make_async_copy(weights, wbuf.at[s], own_sem)
    load_own.start()
    mine = pl.ds(s * share, share)
    loads = [
        pltpu.make_async_copy(stream.at[0, mine], xs.at[0], in_sem.at[0]),
        pltpu.make_async_copy(stream.at[1, mine], xs.at[1], in_sem.at[1]),
        pltpu.make_async_copy(cotangent.at[0, mine], ds.at[0], in_sem.at[2]),
        pltpu.make_async_copy(cotangent.at[1, mine], ds.at[1], in_sem.at[3]),
    ]
    for load in loads:
        load.start()

    zero_row = jnp.zeros((share, 1, W, 3 * C), jnp.bfloat16)
    for k in range(2):
        pads[k, :, 0:1] = zero_row
        pads[k, :, H + 1 : H + 2] = zero_row

    col = lax.rem(lax.broadcasted_iota(jnp.int32, (M, C), 0), W)

    def shifted(k, flat, order):
        before = jnp.where(col == 0, 0.0, pltpu.roll(flat, 1, 0))
        after = jnp.where(col == W - 1, 0.0, pltpu.roll(flat, M - 1, 0))
        for b, piece in enumerate((before, flat, after) if order else (after, flat, before)):
            pads[k, :, 1 : H + 1, :, b * C : (b + 1) * C] = piece.astype(jnp.bfloat16).reshape(
                share, H, W, C)

    def activate(value, sec, which):
        logistic = 1.0 / (1.0 + jnp.exp(-value))
        act = value * logistic
        slopes[sec, which] = logistic * (1.0 + value * (1.0 - logistic))
        kept[sec, which] = act.astype(jnp.bfloat16)
        shifted(0, act, True)

    def conv(sec, which):
        total = jnp.zeros((M, C), jnp.float32)
        for a in range(3):
            total += jnp.dot(
                pads[0, :, a : a + H].reshape(M, 3 * C),
                wbuf[sec, which * 9 * C + a * 3 * C : which * 9 * C + (a + 1) * 3 * C],
                preferred_element_type=jnp.float32)
        return total

    def relay(sec):
        @pl.when((sec != s) & (d < NC))
        def _():
            section_copy(sec, s).wait_recv()
            layer_copy(sec, d, partner).start()

            @pl.loop(1, chips)
            def _(i):
                layer_copy(sec, d, other_chip(i)).start()

    def pass_on(sec):
        @pl.when(sec != s)
        def _():
            @pl.loop(1, chips)
            def _(i):
                src = other_chip(i)

                @pl.when(src < NC)
                def _():
                    layer_copy(sec, src, d).wait_recv()
                    core_copy(sec, src).start()

    def take(sec):
        @pl.when(sec != s)
        def _():
            @pl.when(partner < NC)
            def _():
                layer_copy(sec, partner, d).wait_recv()

            @pl.loop(1, chips)
            def _(i):
                src = lax.rem(partner + 2 * i, D)

                @pl.when(src < NC)
                def _():
                    core_copy(sec, src).wait_recv()

    load_own.wait()
    for load in loads:
        load.wait()
    for sec in range(S):
        relay(sec)
    pass_on(0)

    def forward_one(sec, carry):
        first = xs[0].reshape(M, C)
        second = xs[1].reshape(M, C)
        activate(second, sec, 0)
        take(sec)
        first = first + conv(sec, 0)
        activate(first, sec, 1)
        xs[0] = first.reshape(share, H, W, C)

        @pl.when(sec + 1 < S)
        def _():
            pass_on(sec + 1)

        xs[1] = (second + conv(sec, 1)).reshape(share, H, W, C)
        return carry

    lax.fori_loop(0, S, forward_one, 0)

    def pair_copy(sec, to):
        return pltpu.make_async_remote_copy(
            src_ref=gsend.at[sec, to], dst_ref=pairs.at[sec, to],
            send_sem=psend.at[sec, to], recv_sem=precv.at[sec, to],
            device_id=(s, partner), device_id_type=MESH)

    def grad_copy(sec, src, to):
        return pltpu.make_async_remote_copy(
            src_ref=gsend.at[sec, to], dst_ref=recv1.at[sec, src],
            send_sem=gsend_sem.at[sec, to], recv_sem=grecv_sem.at[sec, src],
            device_id=(s, to), device_id_type=MESH)

    def sum_copy(sec, src):
        return pltpu.make_async_remote_copy(
            src_ref=zsend.at[sec], dst_ref=recv2.at[src],
            send_sem=zsend_sem.at[sec], recv_sem=zrecv_sem.at[src],
            device_id=(sec, d), device_id_type=MESH)

    def grads(sec, which):
        rounded = ds[1 if which else 0].reshape(M, C)
        shifted(1, rounded, False)
        act = kept[sec, which]
        for a in range(3):
            block = lax.dot_general(
                act, pads[1, :, 2 - a : 2 - a + H].reshape(M, 3 * C),
                (((0,), (0,)), ((), ())), preferred_element_type=jnp.float32)
            for b in range(3):
                g32[(3 * a + b) * C : (3 * a + b + 1) * C] = block[:, b * C : (b + 1) * C]
        per = D // 2

        def convert(at):
            gsend[sec, which * per + at] = g32[
                pl.ds(pl.multiple_of(at * rows, 8), rows)].astype(jnp.bfloat16)

        @pl.loop(0, per // 2)
        def _(i):
            at = 2 * i + 1 - core
            convert(at)
            pair_copy(sec, which * per + at).start()

        @pl.loop(0, per // 2)
        def _(i):
            convert(2 * i + core)

        total = jnp.zeros((M, C), jnp.float32)
        for a in range(3):
            for b in range(3):
                tap = 3 * a + b
                total += lax.dot_general(
                    pads[1, :, 2 - a : 2 - a + H, :, b * C : (b + 1) * C].reshape(M, C),
                    wbuf[sec, which * 9 * C + tap * C : which * 9 * C + (tap + 1) * C],
                    (((1,), (1,)), ((), ())), preferred_element_type=jnp.float32)
        into = 0 if which else 1
        ds[into] = ds[into] + (total * slopes[sec, which]).reshape(share, H, W, C)

    def combine(sec, which):
        per = D // 2

        @pl.loop(0, per // 2)
        def _(i):
            to = which * per + 2 * i + core
            pair_copy(sec, to).wait_recv()
            both = gsend[sec, to].astype(jnp.float32) + pairs[sec, to].astype(jnp.float32)
            gsend[sec, to] = both.astype(jnp.bfloat16)

            @pl.when(to != d)
            def _():
                grad_copy(sec, d, to).start()

    def finish(sec):
        def add(i, total):
            src = other_chip(i)
            grad_copy(sec, src, d).wait_recv()
            return total + recv1[sec, src].astype(jnp.float32)

        total = lax.fori_loop(1, chips, add, gsend[sec, d].astype(jnp.float32))

        @pl.when(sec == s)
        def _():
            gown[...] = total

        @pl.when(sec != s)
        def _():
            zsend[sec] = total.astype(jnp.bfloat16)
            sum_copy(sec, s).start()

    def backward_one(turn, carry):
        sec = S - 1 - turn
        grads(sec, 1)
        combine(sec, 1)

        @pl.when(turn > 0)
        def _():
            finish(sec + 1)

        grads(sec, 0)
        combine(sec, 0)
        return carry

    lax.fori_loop(0, S, backward_one, 0)
    finish(0)

    def gather_sums(i, total):
        src = lax.rem(s + i, S)
        sum_copy(s, src).wait_recv()
        return total + recv2[src].astype(jnp.float32)

    summed = lax.fori_loop(1, S, gather_sums, gown[...])
    moved = inertia * momentum[...] + summed / images
    new_momentum[...] = moved
    fresh = master[...] - step_size * moved
    new_master[...] = fresh
    spread_out[d] = fresh.astype(jnp.bfloat16)

    def out_copy(src, to):
        return pltpu.make_async_remote_copy(
            src_ref=spread_out.at[src], dst_ref=spread_out.at[src],
            send_sem=osend_sem.at[to], recv_sem=orecv_sem.at[src],
            device_id=(s, to), device_id_type=MESH)

    def hand_over(src):
        return pltpu.make_async_remote_copy(
            src_ref=spread_out.at[src], dst_ref=spread_out.at[src],
            send_sem=fsend_sem.at[src], recv_sem=frecv_sem.at[src],
            device_id=(s, partner), device_id_type=MESH)

    @pl.loop(1, chips)
    def _(i):
        out_copy(d, other_chip(i)).start()

    out_copy(d, partner).start()

    @pl.loop(1, S)
    def _(i):
        other = lax.rem(s + i, S)
        sum_copy(other, s).wait_send()

        @pl.when(d < NC)
        def _():
            section_copy(s, other).wait_send()
            layer_copy(other, d, partner).wait_send()

        @pl.loop(1, chips)
        def _(j):
            @pl.when(d < NC)
            def _():
                layer_copy(other, d, other_chip(j)).wait_send()

            @pl.when(other_chip(j) < NC)
            def _():
                core_copy(other, other_chip(j)).wait_send()

    @pl.loop(0, S)
    def _(sec):
        @pl.loop(1, chips)
        def _(i):
            grad_copy(sec, d, other_chip(i)).wait_send()

        @pl.loop(0, chips)
        def _(i):
            pair_copy(sec, 2 * i + 1 - core).wait_send()

    @pl.loop(1, chips)
    def _(i):
        src = other_chip(i)
        out_copy(src, d).wait_recv()
        hand_over(src).start()

    out_copy(partner, d).wait_recv()
    out_copy(d, partner).wait_send()

    @pl.loop(1, chips)
    def _(i):
        out_copy(d, other_chip(i)).wait_send()
        hand_over(other_chip(i)).wait_send()
        hand_over(lax.rem(partner + 2 * i, D)).wait_recv()

    new_weights[...] = spread_out[...]


def on_device(S, D, stream, cotangent, weights, master, momentum):
    _, per_dp, H, W, C = stream.shape
    share = per_dp // S
    M = share * H * W
    R = weights.shape[1]
    rows = master.shape[1]
    bf, f32 = jnp.bfloat16, jnp.float32
    vmem = pl.BlockSpec(memory_space=pltpu.VMEM)
    hbm = pl.BlockSpec(memory_space=pl.ANY)
    dma = pltpu.SemaphoreType.DMA
    new_master, new_momentum, new_weights = pl.pallas_call(
        functools.partial(kernel, S, D, per_dp * D),
        out_shape=(
            jax.ShapeDtypeStruct((rows, C), f32),
            jax.ShapeDtypeStruct((rows, C), f32),
            jax.ShapeDtypeStruct((D, rows, C), bf),
        ),
        in_specs=[hbm, hbm, hbm, vmem, vmem],
        out_specs=(vmem, vmem, vmem),
        scratch_shapes=[
            pltpu.VMEM((S, R, C), bf),
            pltpu.VMEM((2, share, H, W, C), f32),
            pltpu.VMEM((2, share, H, W, C), f32),
            pltpu.VMEM((2, share, H + 2, W, 3 * C), bf),
            pltpu.VMEM((S, 2, M, C), bf),
            pltpu.VMEM((S, 2, M, C), f32),
            pltpu.VMEM((R // 2, C), f32),
            pltpu.VMEM((S, D, rows, C), bf),
            pltpu.VMEM((S, D, rows, C), bf),
            pltpu.VMEM((S, D, rows, C), bf),
            pltpu.VMEM((S, rows, C), bf),
            pltpu.VMEM((S, rows, C), bf),
            pltpu.VMEM((rows, C), f32),
            pltpu.VMEM((D, rows, C), bf),
            dma((4,)), dma, dma((S,)), dma((S,)), dma((S, D)), dma((S, D)), dma((S, D)), dma((S, D)),
            dma((S, D)), dma((S, D)), dma((S, D)), dma((S, D)), dma((S,)), dma((S,)),
            dma((D,)), dma((D,)), dma((D,)), dma((D,)),
        ],
        compiler_params=pltpu.CompilerParams(
            has_side_effects=True, vmem_limit_bytes=61 * 1024 * 1024),
    )(stream, cotangent, weights[0], master[0], momentum[0])
    return (new_master[None], new_momentum[None], new_weights.reshape(1, R, C))


def solution(mesh):
    placed = (
        P(None, "dp", None, None, None),
        P(None, "dp", None, None, None),
        P("section", None, None),
        P("section", "dp", None),
        P("section", "dp", None),
    )
    return jax.shard_map(
        functools.partial(on_device, mesh.shape["section"], mesh.shape["dp"]),
        mesh=mesh,
        in_specs=placed,
        out_specs=(P("section", "dp", None), P("section", "dp", None), P("section", None, None)),
        check_vma=False,
    )
```
